16 devices in a mesh: dp: 4 (over y, z, core), tp: 4 (over x).
Axes of the slice: x: 4, y: 2, z: 1, core: 2. Of those that a mesh axis runs over, the one named last changes fastest.
The devices are a block of a 4x4x8 slice.
Arguments:
- x: bfloat16 [16, 512, 5120], P('dp'), parts along dimension 0
- gain_a: bfloat16 [5120], replicated
- wq: bfloat16 [5120, 5120], P(None, 'tp')
- wk: bfloat16 [5120, 5120], P(None, 'tp')
- wv: bfloat16 [5120, 5120], P(None, 'tp')
- wo: bfloat16 [5120, 5120], P('tp')
- gain_m: bfloat16 [5120], replicated
- w_gate: bfloat16 [5120, 13824], P(None, 'tp')
- w_up: bfloat16 [5120, 13824], P(None, 'tp')
- w_down: bfloat16 [13824, 5120], P('tp')
Outputs:
- output: bfloat16 [16, 512, 5120], P('dp'), parts along dimension 0
There are 4 independent parts. The reference program is written for one: setup_inputs(seed, part) draws one part's arguments, and reference() takes and returns one part's arrays. A program takes and returns all parts, laid end to end along the dimension named above; an argument that names none is the same for every part.
All inputs are finite; a program needn't handle non-finite values.
Results may differ from the reference program's by a relative error of at most 0.017.
Values are sent between devices in bfloat16 or wider.
A program may use at most 768 MiB of HBM per device.

```python
import jax
import jax.numpy as jnp
from jax import lax

SEQUENCES = 4
TOKENS = 512
D = 5120
HEADS = 40
KV_HEADS = 40
HEAD = 128
FF = 13824
THETA = 10000


def setup_inputs(seed: int = 0, part: int = 0) -> dict:
    kx, ka, km, kq, kk, kv, ko, kg, ku, kd = jax.random.split(jax.random.key(seed), 10)

    def weights(key, rows, columns):
        return jax.random.normal(key, (rows, columns), jnp.float32) * rows**-0.5

    drawn = {
        "x": jax.random.normal(jax.random.fold_in(kx, part), (SEQUENCES, TOKENS, D), jnp.float32),
        "gain_a": 1 + 0.1 * jax.random.normal(ka, (D,), jnp.float32),
        "wq": 2 * weights(kq, D, HEADS * HEAD),
        "wk": 2 * weights(kk, D, KV_HEADS * HEAD),
        "wv": 4 * weights(kv, D, KV_HEADS * HEAD),
        "wo": weights(ko, HEADS * HEAD, D),
        "gain_m": 1 + 0.1 * jax.random.normal(km, (D,), jnp.float32),
        "w_gate": weights(kg, D, FF),
        "w_up": weights(ku, D, FF),
        "w_down": 3 * weights(kd, FF, D),
    }
    return {k: v.astype(jnp.bfloat16) for k, v in drawn.items()}


def normed(x, gain):
    wide = x.astype(jnp.float32)
    scale = lax.rsqrt(jnp.mean(wide * wide, -1, keepdims=True) + 1e-6)
    return (wide * scale * gain.astype(jnp.float32)).astype(jnp.bfloat16)


def turned(t, place, theta):
    half = t.shape[-1] // 2
    angle = place.astype(jnp.float32)[:, None] * theta ** (-jnp.arange(half, dtype=jnp.float32) / half)
    cos, sin = jnp.cos(angle)[:, None], jnp.sin(angle)[:, None]
    a, b = t[..., :half].astype(jnp.float32), t[..., half:].astype(jnp.float32)
    return jnp.concatenate([a * cos - b * sin, b * cos + a * sin], -1).astype(jnp.bfloat16)


def matmul(a, w):
    return jnp.dot(a, w, preferred_element_type=jnp.float32).astype(jnp.bfloat16)


def einsum(form, a, b):
    return jnp.einsum(form, a.astype(jnp.float32), b.astype(jnp.float32))


def attention(q, k, v):
    scores = einsum("tgsd,ugd->gstu", q, k) * q.shape[-1] ** -0.5
    token = jnp.arange(q.shape[0])
    scores = jnp.where(token[:, None] >= token, scores, -jnp.inf)
    weights = jax.nn.softmax(scores, -1).astype(jnp.bfloat16)
    return einsum("gstu,ugd->tgsd", weights, v).astype(jnp.bfloat16)


def one(x, gain_a, wq, wk, wv, wo, gain_m, w_gate, w_up, w_down):
    rows = x.shape[0]
    a, place = normed(x, gain_a), jnp.arange(rows)
    k = turned(matmul(a, wk).reshape(rows, -1, HEAD), place, THETA)
    q = turned(matmul(a, wq).reshape(rows, -1, HEAD), place, THETA).reshape(rows, k.shape[1], -1, HEAD)
    v = matmul(a, wv).reshape(rows, -1, HEAD)
    seen = attention(q, k, v).reshape(rows, -1)
    h = (x.astype(jnp.float32) + jnp.dot(seen, wo, preferred_element_type=jnp.float32)).astype(jnp.bfloat16)
    b = normed(h, gain_m)
    gate = jnp.dot(b, w_gate, preferred_element_type=jnp.float32)
    up = jnp.dot(b, w_up, preferred_element_type=jnp.float32)
    hidden = (jax.nn.silu(gate) * up).astype(jnp.bfloat16)
    return (h.astype(jnp.float32) + jnp.dot(hidden, w_down, preferred_element_type=jnp.float32)).astype(jnp.bfloat16)


def reference(x, gain_a, wq, wk, wv, wo, gain_m, w_gate, w_up, w_down):
    return lax.map(lambda sequence: one(sequence, gain_a, wq, wk, wv, wo, gain_m, w_gate, w_up, w_down), x)
```

```python
import functools

import jax
import jax.numpy as jnp
import numpy as np
from jax import lax
from jax.experimental import pallas as pl
from jax.experimental.pallas import tpu as pltpu
from jax.sharding import PartitionSpec as P

HEAD = 128
THETA = 10000
TILE = 256
WIDE = 512
STRIP = 16
MESH = pl.DeviceIdType.MESH
F32, BF16 = jnp.float32, jnp.bfloat16


def _dot(a, w):
    return jnp.dot(a, w, preferred_element_type=F32)


def _layer(x, gain_a, wq, wk, wv, wo, gain_m, w_gate, w_up, w_down, cos, sin, out,
           wbuf, vbuf, act, mid, term, got, fin, xin, wsem, vsem, xsem, qsem, osem, send, recv):
    batch, rows, d = x.shape
    units = 2 * batch
    width, ff = wq.shape[1], w_gate.shape[1]
    quarter, half = rows // 4, d // 2
    me = lax.axis_index("tp")
    right, opposite, left = lax.rem(me + 1, 4), lax.rem(me + 2, 4), lax.rem(me + 3, 4)
    low, high, every = pl.ds(0, half), pl.ds(half, half), pl.ds(0, d)

    def of(q):
        return pl.ds(pl.multiple_of(q * quarter, quarter), quarter)

    def unit(u):
        mlp = (u == batch - 1) | (u > batch)
        return mlp, jnp.where(mlp, jnp.where(u == batch - 1, 0, u - batch), jnp.where(u == batch, batch - 1, u))


    def piece(u, n):
        p = lax.rem(u, 2)
        mlp, i = unit(u)
        o = jnp.where(mlp, batch + i, i)
        f = jnp.where(mlp, batch + p, i)
        to = left if n in (0, 1, 2, 6, 8) else right
        if n < 6:
            q, cols = ((opposite, low), (left, high), (left, low), (opposite, high), (right, low), (right, high))[n]
            src, dst = term.at[p, of(q), cols], got.at[p, n]
        elif n < 8:
            src, dst = fin.at[f], out.at[o, of(me), every]
        else:
            q, cols = ((right, low), (left, high))[n - 8]
            src = dst = out.at[o, of(q), cols]
        return pltpu.make_async_remote_copy(src_ref=src, dst_ref=dst, send_sem=send.at[p, n], recv_sem=recv.at[p, n],
                                            device_id={"tp": to}, device_id_type=MESH)

    def residual(u):
        _, i = unit(u)
        return pltpu.make_async_copy(x.at[i, of(me), every], fin.at[i], qsem.at[0])

    def kept(u):
        mlp, i = unit(u)
        return pltpu.make_async_copy(fin.at[jnp.where(mlp, batch + lax.rem(u, 2), i)], out.at[jnp.where(mlp, batch + i, i), of(me), every],
                                     osem.at[lax.rem(u, 2)])

    def begin(u):
        for n in (0, 3, 1, 4):
            piece(u, n).start()
        mlp, _ = unit(u)

        @pl.when(jnp.logical_not(mlp))
        def _():
            residual(u).start()

    def relay(u):
        p = lax.rem(u, 2)
        for n, q, cols, after in ((0, left, low, 2), (3, right, high, 5)):
            piece(u, n).wait_recv()

            def add(r, _):
                here = pl.ds(pl.multiple_of(q * quarter + r * STRIP, STRIP), STRIP)
                came = got[p, n, pl.ds(pl.multiple_of(r * STRIP, STRIP), STRIP), :]
                term[p, here, cols] = (term[p, here, cols].astype(F32) + came.astype(F32)).astype(BF16)

            lax.fori_loop(0, quarter // STRIP, add, None)
            piece(u, after).start()

    def own(u):
        p = lax.rem(u, 2)
        mlp, i = unit(u)
        f = jnp.where(mlp, batch + p, i)
        for n in (1, 4, 2, 5):
            piece(u, n).wait_recv()

        @pl.when(jnp.logical_not(mlp))
        def _():
            residual(u).wait()

        def add(r, _):
            here = pl.ds(pl.multiple_of(r * STRIP, STRIP), STRIP)
            mine = pl.ds(pl.multiple_of(me * quarter + r * STRIP, STRIP), STRIP)
            for cols, a, b in ((low, 2, 4), (high, 5, 1)):
                total = term[p, mine, cols].astype(F32) + got[p, a, here, :].astype(F32) + got[p, b, here, :].astype(F32)
                fin[f, here, cols] = (fin[i, here, cols].astype(F32) + total).astype(BF16)

        lax.fori_loop(0, quarter // STRIP, add, None)
        for n in (6, 7):
            piece(u, n).start()
        kept(u).start()

    def forward(u):
        for n, after in ((6, 8), (7, 9)):
            piece(u, n).wait_recv()
            piece(u, after).start()
        for n in range(6):
            piece(u, n).wait_send()

    def end(u):
        for n in (8, 9):
            piece(u, n).wait_recv()
        for n in (6, 7, 8, 9):
            piece(u, n).wait_send()
        kept(u).wait()

    def when(u, *events):
        @pl.when((u >= 0) & (u < units))
        def _():
            for event in events:
                event(u)


    def norm(src, i, gain):
        part = xin.shape[1]

        def load(t):
            return pltpu.make_async_copy(src.at[i, pl.ds(pl.multiple_of(t * part, part), part), every], xin.at[lax.rem(t, 2)],
                                         xsem.at[lax.rem(t, 2)])

        load(0).start()
        g = gain[...].astype(F32)

        def tile(t, _):
            @pl.when(t + 1 < rows // part)
            def _():
                load(t + 1).start()

            load(t).wait()

            def strip(r, _):
                wide = xin[lax.rem(t, 2), pl.ds(pl.multiple_of(r * STRIP, STRIP), STRIP), :].astype(F32)
                scale = lax.rsqrt(jnp.mean(wide * wide, -1, keepdims=True) + 1e-6)
                act[pl.ds(pl.multiple_of(t * part + r * STRIP, STRIP), STRIP), :] = (wide * scale * g).astype(BF16)

            lax.fori_loop(0, part // STRIP, strip, None)

        lax.fori_loop(0, rows // part, tile, None)

    def tiled(count, start, wait, work, hook=None):
        def step(j, _):
            @pl.when(j + 1 < count)
            def _():
                start(j + 1)

            wait(j)
            work(j)
            if hook is not None:
                pl.when(j == hook[0])(hook[1])

        lax.fori_loop(0, count, step, None)

    def last_start(w):
        def copy(j):
            depth = w.shape[0]
            return pltpu.make_async_copy(w.at[:, pl.ds(pl.multiple_of(j * WIDE, WIDE), WIDE)], vbuf.at[lax.rem(j, 2), pl.ds(0, depth), :],
                                         vsem.at[lax.rem(j, 2)])
        return copy

    def last(w, p):
        depth = w.shape[0]
        copy = last_start(w)

        def work(j):
            term[p, :, pl.ds(pl.multiple_of(j * WIDE, WIDE), WIDE)] = _dot(mid[:, :depth], vbuf[lax.rem(j, 2), :depth, :]).astype(BF16)

        tiled(d // WIDE, lambda j: copy(j).start(), lambda j: copy(j).wait(), work)

    def turn(t):
        t = t.astype(F32)
        return (t * cos[...] + pltpu.roll(t, HEAD // 2, 1) * sin[...]).astype(BF16)

    def head(n, _):
        at = [pl.ds(pl.multiple_of(k * width + n * HEAD, HEAD), HEAD) for k in range(3)]
        q, k, v = turn(mid[:, at[0]]), turn(mid[:, at[1]]), mid[:, at[2]]
        size = rows // 2
        for first in (0, size):
            keys = first + size
            s = lax.dot_general(q[first:keys], k[:keys], (((1,), (1,)), ((), ())), preferred_element_type=F32) * HEAD**-0.5
            seen = first + lax.broadcasted_iota(jnp.int32, (size, keys), 0) >= lax.broadcasted_iota(jnp.int32, (size, keys), 1)
            s = jnp.where(seen, s, -1e30)
            w = jnp.exp(s - s.max(-1, keepdims=True))
            total = w.sum(-1, keepdims=True)
            mid[first:keys, at[0]] = (_dot(w.astype(BF16), v[:keys]) * (1 / total)).astype(BF16)

    def attention_unit(i, p, early, late):
        per = width // TILE

        def start(j):
            for k, w in enumerate((wq, wk, wv)):
                @pl.when(lax.div(j, per) == k)
                def _():
                    cols = pl.ds(pl.multiple_of(lax.rem(j, per) * TILE, TILE), TILE)
                    pltpu.make_async_copy(w.at[:, cols], wbuf.at[lax.rem(j, 2)], wsem.at[lax.rem(j, 2), 0]).start()

        def wait(j):
            pltpu.make_async_copy(wq.at[:, pl.ds(0, TILE)], wbuf.at[lax.rem(j, 2)], wsem.at[lax.rem(j, 2), 0]).wait()

        def work(j):
            mid[:, pl.ds(pl.multiple_of(j * TILE, TILE), TILE)] = _dot(act[...], wbuf[lax.rem(j, 2)]).astype(BF16)

        start(0)
        last_start(wo)(0).start()
        norm(x, i, gain_a)
        tiled(3 * per, start, wait, work, (3 * per // 2, early))
        lax.fori_loop(0, width // HEAD, head, None)
        late()
        last(wo, p)

    def mlp_unit(i, p, early, late):
        part = TILE // 2

        def copies(j):
            cols = pl.ds(pl.multiple_of(j * part, part), part)
            return [pltpu.make_async_copy(w.at[:, cols], wbuf.at[lax.rem(j, 2), :, pl.ds(k * part, part)], wsem.at[lax.rem(j, 2), k])
                    for k, w in enumerate((w_gate, w_up))]

        def work(j):
            both = _dot(act[...], wbuf[lax.rem(j, 2)])
            mid[:, pl.ds(pl.multiple_of(j * part, part), part)] = (jax.nn.silu(both[:, :part]) * both[:, part:]).astype(BF16)

        def start(j):
            for c in copies(j):
                c.start()

        def wait(j):
            for c in copies(j):
                c.wait()

        count = ff // part

        def hooks(j):
            pass

        start(0)
        last_start(w_down)(0).start()
        norm(out, i, gain_m)

        def both_hooks(j):
            pl.when(j == count // 4)(early)
            pl.when(j == count - 1)(late)

        def work_and_hooks(j):
            work(j)
            both_hooks(j)

        tiled(count, start, wait, work_and_hooks)
        last(w_down, p)


    barrier = pltpu.get_barrier_semaphore()
    for neighbour in (left, right):
        pl.semaphore_signal(barrier, inc=1, device_id={"tp": neighbour}, device_id_type=MESH)
    pl.semaphore_wait(barrier, 2)

    def slot(s, _):
        mlp, i = unit(s)
        p = lax.rem(s, 2)

        def early():
            when(s - 1, relay)
            when(s - 2, forward)

        def late():
            when(s - 1, own)

        when(s - 1, begin)

        @pl.when((s < units) & jnp.logical_not(mlp))
        def _():
            attention_unit(i, p, early, late)

        @pl.when((s < units) & mlp)
        def _():
            mlp_unit(i, p, early, late)

        @pl.when(s >= units)
        def _():
            early()
            late()

        when(s - 2, end)

    lax.fori_loop(0, units + 2, slot, None)


def layer(x, gain_a, wq, wk, wv, wo, gain_m, w_gate, w_up, w_down):
    batch, rows, d = x.shape
    width, ff = wq.shape[1], w_gate.shape[1]
    half = HEAD // 2
    angle = np.arange(rows, dtype=np.float32)[:, None] * np.power(np.float32(THETA), -np.arange(half, dtype=np.float32) / np.float32(half))
    cos, sin = np.cos(angle).astype(np.float32), np.sin(angle).astype(np.float32)
    cos, sin = np.concatenate([cos, cos], 1), np.concatenate([-sin, sin], 1)
    hbm, vmem = pl.BlockSpec(memory_space=pl.ANY), pl.BlockSpec(memory_space=pltpu.VMEM)
    part = min(rows, 128)
    out = pl.pallas_call(
        _layer,
        in_specs=[hbm, vmem, hbm, hbm, hbm, hbm, vmem, hbm, hbm, hbm, vmem, vmem],
        out_specs=hbm,
        out_shape=jax.ShapeDtypeStruct((2 * batch, rows, d), BF16),
        scratch_shapes=[
            pltpu.VMEM((2, d, TILE), BF16),
            pltpu.VMEM((2, max(width, ff), WIDE), BF16),
            pltpu.VMEM((rows, d), BF16),
            pltpu.VMEM((rows, max(3 * width, ff)), BF16),
            pltpu.VMEM((2, rows, d), BF16),
            pltpu.VMEM((2, 6, rows // 4, d // 2), BF16),
            pltpu.VMEM((batch + 2, rows // 4, d), BF16),
            pltpu.VMEM((2, part, d), BF16),
            pltpu.SemaphoreType.DMA((2, 2)),
            pltpu.SemaphoreType.DMA((2,)),
            pltpu.SemaphoreType.DMA((2,)),
            pltpu.SemaphoreType.DMA((1,)),
            pltpu.SemaphoreType.DMA((2,)),
            pltpu.SemaphoreType.DMA((2, 10)),
            pltpu.SemaphoreType.DMA((2, 10)),
        ],
        compiler_params=pltpu.CompilerParams(collective_id=0, has_side_effects=True, vmem_limit_bytes=67043328),
        name="layer",
    )(x, gain_a.reshape(1, d), wq, wk, wv, wo, gain_m.reshape(1, d), w_gate, w_up, w_down, jnp.asarray(cos), jnp.asarray(sin))
    return out[batch:]


def solution(mesh):
    tokens, whole, columns, rows_of = P("dp", None, None), P(None), P(None, "tp"), P("tp", None)
    return jax.shard_map(
        layer,
        mesh=mesh,
        in_specs=(tokens, whole, columns, columns, columns, rows_of, whole, columns, columns, rows_of),
        out_specs=tokens,
        check_vma=False,
    )
```

```python
import functools

import jax
import jax.numpy as jnp
import numpy as np
from jax import lax
from jax.experimental import pallas as pl
from jax.experimental.pallas import tpu as pltpu
from jax.sharding import PartitionSpec as P

HEAD = 128
THETA = 10000
SLOTS = 4
TILE = 256
WIDE = 512
STRIP = 16
COPIED = 256
EARLY, LATE = (8, 5, 8), (16, 14, 16)
MESH = pl.DeviceIdType.MESH
F32, BF16 = jnp.float32, jnp.bfloat16


def _dot(a, w):
    return jnp.dot(a, w, preferred_element_type=F32)


def _layer(x, gains, wq, wk, wv, wo, w_gate, w_up, w_down, cos, sin, out,
           wbuf, vbuf, act, mid, term, got, fin, xin, wsem, vsem, xsem, qsem, osem, send, recv):
    batch, rows, d = x.shape
    units = 2 * batch + 1
    width, ff = wq.shape[1], w_gate.shape[1]
    block, half = rows // 2, d // 2
    me = lax.axis_index("tp")
    right, opposite, left = lax.rem(me + 1, 4), lax.rem(me + 2, 4), lax.rem(me + 3, 4)
    low, high, every = pl.ds(0, half), pl.ds(half, half), pl.ds(0, d)

    def unit(u):
        mlp = (u == batch) | (u > batch + 1)
        return mlp, jnp.where(mlp, jnp.where(u == batch, 0, u - 1 - batch), jnp.where(u == batch + 1, batch - 1, jnp.maximum(u - 1, 0)))

    def share(small):
        return (block if small else rows) // 4

    def of(q, small):
        return pl.ds(pl.multiple_of(q * share(small), share(small)), share(small))

    def at(u, q, small):
        first = u * block if small else 0
        return pl.ds(pl.multiple_of(first + q * share(small), share(small)), share(small))


    def piece(u, n, small):
        p = lax.rem(u, 2)
        mlp, i = unit(u)
        o = jnp.where(mlp, batch + i, i)
        to = left if n in (0, 1, 2, 6, 8, 10) else right
        some = pl.ds(0, share(small))
        if n < 6:
            q, cols = ((opposite, low), (left, high), (left, low), (opposite, high), (right, low), (right, high))[n]
            src, dst = term.at[p, of(q, small), cols], got.at[p, n, some]
        elif n in (6, 7, 10, 11):
            cols = low if n in (6, 11) else high
            src, dst = fin.at[p, some, cols], out.at[o, at(u, me, small), cols]
        else:
            q, cols = ((right, low), (left, high))[n - 8]
            src = dst = out.at[o, at(u, q, small), cols]
        return pltpu.make_async_remote_copy(src_ref=src, dst_ref=dst, send_sem=send.at[p, n], recv_sem=recv.at[p, n],
                                            device_id={"tp": to}, device_id_type=MESH)

    def residual(u, small, src):
        _, i = unit(u)
        return pltpu.make_async_copy(src.at[i, at(u, me, small), every], fin.at[lax.rem(u, 2), pl.ds(0, share(small))], qsem.at[0])

    def kept(u, small):
        mlp, i = unit(u)
        p = lax.rem(u, 2)
        return pltpu.make_async_copy(fin.at[p, pl.ds(0, share(small))], out.at[jnp.where(mlp, batch + i, i), at(u, me, small), every], osem.at[p])

    def begin(u, small):
        for n in (0, 3, 1, 4):
            piece(u, n, small).start()
        if small:
            residual(u, small, x).start()
        else:
            mlp, _ = unit(u)

            @pl.when(mlp)
            def _():
                residual(u, small, out).start()

            @pl.when(jnp.logical_not(mlp))
            def _():
                residual(u, small, x).start()

    def relay(u, small):
        p = lax.rem(u, 2)
        for n, q, cols, after in ((0, left, low, 2), (3, right, high, 5)):
            piece(u, n, small).wait_recv()

            def add(r, _):
                here = pl.ds(pl.multiple_of(q * share(small) + r * STRIP, STRIP), STRIP)
                came = got[p, n, pl.ds(pl.multiple_of(r * STRIP, STRIP), STRIP), :]
                term[p, here, cols] = (term[p, here, cols].astype(F32) + came.astype(F32)).astype(BF16)

            lax.fori_loop(0, share(small) // STRIP, add, None)
            piece(u, after, small).start()

    def own(u, small):
        p = lax.rem(u, 2)
        for n in (1, 4, 2, 5):
            piece(u, n, small).wait_recv()
        residual(u, small, x).wait()

        def add(r, _):
            here = pl.ds(pl.multiple_of(r * STRIP, STRIP), STRIP)
            mine = pl.ds(pl.multiple_of(me * share(small) + r * STRIP, STRIP), STRIP)
            for cols, a, b in ((low, 2, 4), (high, 5, 1)):
                total = term[p, mine, cols].astype(F32) + got[p, a, here, :].astype(F32) + got[p, b, here, :].astype(F32)
                fin[p, here, cols] = (fin[p, here, cols].astype(F32) + total).astype(BF16)

        lax.fori_loop(0, share(small) // STRIP, add, None)
        for n in (6, 7, 10, 11):
            piece(u, n, small).start()
        kept(u, small).start()

    def forward(u, small):
        for n, after in ((6, 8), (7, 9)):
            piece(u, n, small).wait_recv()
            piece(u, after, small).start()
        for n in range(6):
            piece(u, n, small).wait_send()

    def end(u, small):
        for n in (10, 11, 8, 9):
            piece(u, n, small).wait_recv()
        for n in (6, 7, 10, 11, 8, 9):
            piece(u, n, small).wait_send()
        kept(u, small).wait()

    def when(u, event):
        @pl.when((u >= 0) & (u < 2))
        def _():
            event(u, True)

        @pl.when((u >= 2) & (u < units))
        def _():
            event(u, False)


    def norm(src, i, first, size, gain, then):
        part = min(xin.shape[1], size)

        def load(t):
            return pltpu.make_async_copy(src.at[i, pl.ds(pl.multiple_of(first + t * part, part), part), every],
                                         xin.at[lax.rem(t, 2), pl.ds(0, part)], xsem.at[lax.rem(t, 2)])

        load(0).start()
        then()
        g = gains[gain : gain + 1, :].astype(F32)

        def tile(t, _):
            @pl.when(t + 1 < size // part)
            def _():
                load(t + 1).start()

            load(t).wait()

            def strip(r, _):
                wide = xin[lax.rem(t, 2), pl.ds(pl.multiple_of(r * STRIP, STRIP), STRIP), :].astype(F32)
                scale = lax.rsqrt(jnp.mean(wide * wide, -1, keepdims=True) + 1e-6)
                act[pl.ds(pl.multiple_of(t * part + r * STRIP, STRIP), STRIP), :] = (wide * scale * g).astype(BF16)

            lax.fori_loop(0, part // STRIP, strip, None)

        lax.fori_loop(0, size // part, tile, None)

    def tiled(count, slots, start, wait, work, hooks=()):
        def step(j, _):
            @pl.when(j + slots - 1 < count)
            def _():
                start(j + slots - 1)

            wait(j)
            work(j)
            for when_j, hook in hooks:
                pl.when(j == when_j)(hook)

        lax.fori_loop(0, count, step, None)

    def last_slots(w):
        return 2 * (vbuf.shape[1] // w.shape[0])

    def last_at(w, j):
        slot, depth = lax.rem(j, last_slots(w)), w.shape[0]
        return lax.rem(slot, 2), pl.ds(pl.multiple_of(lax.div(slot, 2) * depth, depth), depth), slice(None)

    def last_tile(w, j):
        return pltpu.make_async_copy(w.at[:, pl.ds(pl.multiple_of(j * WIDE, WIDE), WIDE)], vbuf.at[last_at(w, j)],
                                     vsem.at[lax.rem(j, last_slots(w))])

    def last_begin(w):
        for j in range(last_slots(w) - 1):
            last_tile(w, j).start()

    def last(w, p, first, size):
        def work(j):
            term[p, :size, pl.ds(pl.multiple_of(j * WIDE, WIDE), WIDE)] = _dot(mid[first : first + size, : w.shape[0]],
                                                                               vbuf[last_at(w, j)]).astype(BF16)

        tiled(d // WIDE, last_slots(w), lambda j: last_tile(w, j).start(), lambda j: last_tile(w, j).wait(), work)

    def turn(t, where):
        t = t.astype(F32)
        return (t * cos[where] + pltpu.roll(t, HEAD // 2, 1) * sin[where]).astype(BF16)

    def attend(firsts):
        def head(n, _):
            cols = [pl.ds(pl.multiple_of(k * width + n * HEAD, HEAD), HEAD) for k in range(3)]
            most = firsts[-1] + block
            k, v = turn(mid[:most, cols[1]], slice(0, most)), mid[:most, cols[2]]
            for first in firsts:
                keys = first + block
                q = turn(mid[first:keys, cols[0]], slice(first, keys))
                s = lax.dot_general(q, k[:keys], (((1,), (1,)), ((), ())), preferred_element_type=F32) * HEAD**-0.5
                seen = first + lax.broadcasted_iota(jnp.int32, (block, keys), 0) >= lax.broadcasted_iota(jnp.int32, (block, keys), 1)
                s = jnp.where(seen, s, -1e30)
                w = jnp.exp(s - s.max(-1, keepdims=True))
                total = w.sum(-1, keepdims=True)
                mid[first:keys, cols[0]] = (_dot(w.astype(BF16), v[:keys]) * (1 / total)).astype(BF16)

        lax.fori_loop(0, width // HEAD, head, None)

    def attention_unit(i, p, firsts, early, late, early_at, late_at):
        per = width // TILE
        first, size = firsts[0], len(firsts) * block

        def start(j):
            for k, w in enumerate((wq, wk, wv)):
                @pl.when(lax.div(j, per) == k)
                def _():
                    cols = pl.ds(pl.multiple_of(lax.rem(j, per) * TILE, TILE), TILE)
                    pltpu.make_async_copy(w.at[:, cols], wbuf.at[lax.rem(j, SLOTS)], wsem.at[lax.rem(j, SLOTS), 0]).start()

        def wait(j):
            pltpu.make_async_copy(wq.at[:, pl.ds(0, TILE)], wbuf.at[lax.rem(j, SLOTS)], wsem.at[lax.rem(j, SLOTS), 0]).wait()

        def work(j):
            mid[first : first + size, pl.ds(pl.multiple_of(j * TILE, TILE), TILE)] = _dot(act[:size, :], wbuf[lax.rem(j, SLOTS)]).astype(BF16)

        def ahead():
            for j in range(SLOTS - 1):
                start(j)
            last_begin(wo)

        norm(x, i, first, size, 0, ahead)
        tiled(3 * per, SLOTS, start, wait, work, ((early_at, early), (late_at, late)))
        attend(firsts)
        pl.when(late_at >= 3 * per)(late)
        last(wo, p, first, size)

    def mlp_unit(i, p, early, late):
        part = TILE // 2
        count = ff // part

        def copies(j):
            cols = pl.ds(pl.multiple_of(j * part, part), part)
            return [pltpu.make_async_copy(w.at[:, cols], wbuf.at[lax.rem(j, SLOTS), :, pl.ds(k * part, part)], wsem.at[lax.rem(j, SLOTS), k])
                    for k, w in enumerate((w_gate, w_up))]

        def work(j):
            both = _dot(act[...], wbuf[lax.rem(j, SLOTS)])
            mid[:, pl.ds(pl.multiple_of(j * part, part), part)] = (jax.nn.silu(both[:, :part]) * both[:, part:]).astype(BF16)

        def start(j):
            for c in copies(j):
                c.start()

        def wait(j):
            for c in copies(j):
                c.wait()

        def ahead():
            for j in range(SLOTS - 1):
                start(j)
            last_begin(w_down)

        norm(out, i, 0, rows, 1, ahead)
        tiled(count, SLOTS, start, wait, work, ((count // 4, early), (count - 1, late)))
        last(w_down, p, 0, rows)


    def nothing():
        pass

    steps = 3 * (width // TILE)
    barrier = pltpu.get_barrier_semaphore()
    for neighbour in (left, right):
        pl.semaphore_signal(barrier, inc=1, device_id={"tp": neighbour}, device_id_type=MESH)
    attention_unit(0, 0, (0,), nothing, nothing, steps, steps)
    pl.semaphore_wait(barrier, 2)
    begin(0, True)
    attention_unit(0, 1, (block,), lambda: relay(0, True), lambda: own(0, True), EARLY[0] * steps // 16, LATE[0] * steps // 16)

    def slot(s, _):
        mlp, i = unit(s)
        p = lax.rem(s, 2)

        def early():
            when(s - 1, relay)
            when(s - 2, forward)

        def late():
            when(s - 1, own)

        when(s - 1, begin)

        @pl.when((s < units) & jnp.logical_not(mlp))
        def _():
            attention_unit(i, p, (0, block), early, late, jnp.where(s == 2, EARLY[1] * steps // 16, EARLY[2] * steps // 16),
                           jnp.where(s == 2, LATE[1] * steps // 16, LATE[2] * steps // 16))

        @pl.when((s < units) & mlp)
        def _():
            mlp_unit(i, p, early, late)

        @pl.when(s >= units)
        def _():
            early()
            late()

        when(s - 2, end)

    lax.fori_loop(2, units + 2, slot, None)


def _copy(src, dst, buf, came, left):
    batch, rows, _ = dst.shape
    part = buf.shape[1]
    places = [(i, pl.ds(r * part, part)) for i in range(batch) for r in range(rows // part)]

    def into(n):
        i, here = places[n]
        return pltpu.make_async_copy(src.at[src.shape[0] - batch + i, here], buf.at[n], came.at[n])

    def back(n):
        i, here = places[n]
        return pltpu.make_async_copy(buf.at[n], dst.at[i, here], left.at[n])

    for n in range(len(places)):
        into(n).start()
    for n in range(len(places)):
        into(n).wait()
        back(n).start()
    for n in range(len(places)):
        back(n).wait()


def layer(x, gain_a, wq, wk, wv, wo, gain_m, w_gate, w_up, w_down):
    batch, rows, d = x.shape
    width, ff = wq.shape[1], w_gate.shape[1]
    half = HEAD // 2
    angle = np.arange(rows, dtype=np.float32)[:, None] * np.power(np.float32(THETA), -np.arange(half, dtype=np.float32) / np.float32(half))
    cos, sin = np.cos(angle).astype(np.float32), np.sin(angle).astype(np.float32)
    cos, sin = np.concatenate([cos, cos], 1), np.concatenate([-sin, sin], 1)
    hbm, vmem = pl.BlockSpec(memory_space=pl.ANY), pl.BlockSpec(memory_space=pltpu.VMEM)
    part = min(rows // 2, 128)
    out = pl.pallas_call(
        _layer,
        in_specs=[hbm, vmem, hbm, hbm, hbm, hbm, hbm, hbm, hbm, vmem, vmem],
        out_specs=hbm,
        out_shape=jax.ShapeDtypeStruct((2 * batch, rows, d), BF16),
        scratch_shapes=[
            pltpu.VMEM((SLOTS, d, TILE), BF16),
            pltpu.VMEM((2, max(width, ff), WIDE), BF16),
            pltpu.VMEM((rows, d), BF16),
            pltpu.VMEM((rows, max(3 * width, ff)), BF16),
            pltpu.VMEM((2, rows, d), BF16),
            pltpu.VMEM((2, 6, rows // 4, d // 2), BF16),
            pltpu.VMEM((2, rows // 4, d), BF16),
            pltpu.VMEM((2, part, d), BF16),
            pltpu.SemaphoreType.DMA((SLOTS, 2)),
            pltpu.SemaphoreType.DMA((2 * (max(width, ff) // min(width, ff)),)),
            pltpu.SemaphoreType.DMA((2,)),
            pltpu.SemaphoreType.DMA((1,)),
            pltpu.SemaphoreType.DMA((2,)),
            pltpu.SemaphoreType.DMA((2, 12)),
            pltpu.SemaphoreType.DMA((2, 12)),
        ],
        compiler_params=pltpu.CompilerParams(collective_id=0, has_side_effects=True, vmem_limit_bytes=67043328),
        name="layer",
    )(x, jnp.stack([gain_a, gain_m]), wq, wk, wv, wo, w_gate, w_up, w_down, jnp.asarray(cos), jnp.asarray(sin))
    part = min(rows, COPIED)
    parts = batch * rows // part
    return pl.pallas_call(
        _copy,
        in_specs=[hbm],
        out_specs=hbm,
        out_shape=jax.ShapeDtypeStruct((batch, rows, d), BF16),
        scratch_shapes=[pltpu.VMEM((parts, part, d), BF16), pltpu.SemaphoreType.DMA((parts,)), pltpu.SemaphoreType.DMA((parts,))],
        compiler_params=pltpu.CompilerParams(vmem_limit_bytes=48 * 2**20),
        name="result",
    )(out)


def solution(mesh):
    tokens, whole, columns, rows_of = P("dp", None, None), P(None), P(None, "tp"), P("tp", None)
    return jax.shard_map(
        layer,
        mesh=mesh,
        in_specs=(tokens, whole, columns, columns, columns, rows_of, whole, columns, columns, rows_of),
        out_specs=tokens,
        check_vma=False,
    )
```

```python
import functools

import jax
import jax.numpy as jnp
import numpy as np
from jax import lax
from jax.experimental import pallas as pl
from jax.experimental.pallas import tpu as pltpu
from jax.sharding import PartitionSpec as P

HEAD = 128
THETA = 10000
GROUP = 5
SLOTS = 4
TILE = 256
WIDE = 512
STRIP = 16
COPIED = 256
EARLY, LATE = (8, 5, 8), (16, 14, 16)
MESH = pl.DeviceIdType.MESH
F32, BF16 = jnp.float32, jnp.bfloat16


def _dot(a, w):
    return jnp.dot(a, w, preferred_element_type=F32)


def _layer(x, gain_a, wq, wk, wv, wo, gain_m, w_gate, w_up, w_down, tables, out,
           turns, tsem, wbuf, vbuf, act, mid, term, got, fin, xin, wsem, vsem, xsem, qsem, osem, send, recv):
    batch, rows, d = x.shape
    units = 2 * batch + 1
    width, ff = wq.shape[1], w_gate.shape[1]
    block, half = rows // 2, d // 2
    me = lax.axis_index("tp")
    right, opposite, left = lax.rem(me + 1, 4), lax.rem(me + 2, 4), lax.rem(me + 3, 4)
    low, high, every = pl.ds(0, half), pl.ds(half, half), pl.ds(0, d)

    def unit(u):
        mlp = (u == batch) | (u > batch + 1)
        return mlp, jnp.where(mlp, jnp.where(u == batch, 0, u - 1 - batch), jnp.where(u == batch + 1, batch - 1, jnp.maximum(u - 1, 0)))

    def share(small):
        return (block if small else rows) // 4

    def of(q, small):
        return pl.ds(pl.multiple_of(q * share(small), share(small)), share(small))

    def at(u, q, small):
        first = u * block if small else 0
        return pl.ds(pl.multiple_of(first + q * share(small), share(small)), share(small))


    def piece(u, n, small):
        p = lax.rem(u, 2)
        mlp, i = unit(u)
        o = jnp.where(mlp, batch + i, i)
        to = left if n in (0, 1, 2, 6, 8, 10) else right
        some = pl.ds(0, share(small))
        if n < 6:
            q, cols = ((opposite, low), (left, high), (left, low), (opposite, high), (right, low), (right, high))[n]
            src, dst = term.at[p, of(q, small), cols], got.at[p, n, some]
        elif n in (6, 7, 10, 11):
            cols = low if n in (6, 11) else high
            src, dst = fin.at[p, some, cols], out.at[o, at(u, me, small), cols]
        else:
            q, cols = ((right, low), (left, high))[n - 8]
            src = dst = out.at[o, at(u, q, small), cols]
        return pltpu.make_async_remote_copy(src_ref=src, dst_ref=dst, send_sem=send.at[p, n], recv_sem=recv.at[p, n],
                                            device_id={"tp": to}, device_id_type=MESH)

    def residual(u, small, src):
        _, i = unit(u)
        return pltpu.make_async_copy(src.at[i, at(u, me, small), every], fin.at[lax.rem(u, 2), pl.ds(0, share(small))], qsem.at[0])

    def kept(u, small):
        mlp, i = unit(u)
        p = lax.rem(u, 2)
        return pltpu.make_async_copy(fin.at[p, pl.ds(0, share(small))], out.at[jnp.where(mlp, batch + i, i), at(u, me, small), every], osem.at[p])

    def begin(u, small):
        for n in (0, 3, 1, 4):
            piece(u, n, small).start()
        if small:
            residual(u, small, x).start()
        else:
            mlp, _ = unit(u)

            @pl.when(mlp)
            def _():
                residual(u, small, out).start()

            @pl.when(jnp.logical_not(mlp))
            def _():
                residual(u, small, x).start()

    def relay(u, small):
        p = lax.rem(u, 2)
        for n, q, cols, after in ((0, left, low, 2), (3, right, high, 5)):
            piece(u, n, small).wait_recv()

            def add(r, _):
                here = pl.ds(pl.multiple_of(q * share(small) + r * STRIP, STRIP), STRIP)
                came = got[p, n, pl.ds(pl.multiple_of(r * STRIP, STRIP), STRIP), :]
                term[p, here, cols] = (term[p, here, cols].astype(F32) + came.astype(F32)).astype(BF16)

            lax.fori_loop(0, share(small) // STRIP, add, None)
            piece(u, after, small).start()

    def own(u, small):
        p = lax.rem(u, 2)
        for n in (1, 4, 2, 5):
            piece(u, n, small).wait_recv()
        residual(u, small, x).wait()

        def add(r, _):
            here = pl.ds(pl.multiple_of(r * STRIP, STRIP), STRIP)
            mine = pl.ds(pl.multiple_of(me * share(small) + r * STRIP, STRIP), STRIP)
            for cols, a, b in ((low, 2, 4), (high, 5, 1)):
                total = term[p, mine, cols].astype(F32) + got[p, a, here, :].astype(F32) + got[p, b, here, :].astype(F32)
                fin[p, here, cols] = (fin[p, here, cols].astype(F32) + total).astype(BF16)

        lax.fori_loop(0, share(small) // STRIP, add, None)
        for n in (6, 7, 10, 11):
            piece(u, n, small).start()
        kept(u, small).start()

    def forward(u, small):
        for n, after in ((6, 8), (7, 9)):
            piece(u, n, small).wait_recv()
            piece(u, after, small).start()
        for n in range(6):
            piece(u, n, small).wait_send()

    def end(u, small):
        for n in (10, 11, 8, 9):
            piece(u, n, small).wait_recv()
        for n in (6, 7, 10, 11, 8, 9):
            piece(u, n, small).wait_send()
        kept(u, small).wait()

    def when(u, event):
        @pl.when((u >= 0) & (u < 2))
        def _():
            event(u, True)

        @pl.when((u >= 2) & (u < units))
        def _():
            event(u, False)


    def norm(src, i, first, size, gain, then):
        part = min(xin.shape[1], size)

        def load(t):
            return pltpu.make_async_copy(src.at[i, pl.ds(pl.multiple_of(first + t * part, part), part), every],
                                         xin.at[lax.rem(t, 2), pl.ds(0, part)], xsem.at[lax.rem(t, 2)])

        load(0).start()
        if size > part:
            load(1).start()
        then()
        g = gain[...].astype(F32).reshape(1, d)

        def tile(t, _):
            @pl.when((t >= 1) & (t + 1 < size // part))
            def _():
                load(t + 1).start()

            load(t).wait()

            def strip(r, _):
                wide = xin[lax.rem(t, 2), pl.ds(pl.multiple_of(r * STRIP, STRIP), STRIP), :].astype(F32)
                scale = lax.rsqrt(jnp.mean(wide * wide, -1, keepdims=True) + 1e-6)
                act[pl.ds(pl.multiple_of(t * part + r * STRIP, STRIP), STRIP), :] = (wide * scale * g).astype(BF16)

            lax.fori_loop(0, part // STRIP, strip, None, unroll=2)

        lax.fori_loop(0, size // part, tile, None)

    def tiled(count, slots, start, wait, work, hooks=()):
        def step(j, _):
            @pl.when(j + slots - 1 < count)
            def _():
                start(j + slots - 1)

            wait(j)
            work(j)
            for when_j, hook in hooks:
                pl.when(j == when_j)(hook)

        lax.fori_loop(0, count, step, None)

    def last_slots(w):
        return 2 * (vbuf.shape[1] // w.shape[0])

    def last_at(w, j):
        slot, depth = lax.rem(j, last_slots(w)), w.shape[0]
        return lax.rem(slot, 2), pl.ds(pl.multiple_of(lax.div(slot, 2) * depth, depth), depth), slice(None)

    def last_tile(w, j):
        return pltpu.make_async_copy(w.at[:, pl.ds(pl.multiple_of(j * WIDE, WIDE), WIDE)], vbuf.at[last_at(w, j)],
                                     vsem.at[lax.rem(j, last_slots(w))])

    def last_begin(w):
        for j in range(last_slots(w) - 1):
            last_tile(w, j).start()

    def last(w, p, first, size):
        def work(j):
            term[p, :size, pl.ds(pl.multiple_of(j * WIDE, WIDE), WIDE)] = _dot(mid[first : first + size, : w.shape[0]],
                                                                               vbuf[last_at(w, j)]).astype(BF16)

        tiled(d // WIDE, last_slots(w), lambda j: last_tile(w, j).start(), lambda j: last_tile(w, j).wait(), work)

    def turn(t, where):
        t = t.astype(F32)
        return (t * turns[0, where] + pltpu.roll(t, HEAD // 2, 1) * turns[1, where]).astype(BF16)

    def attend(firsts, group):
        most = firsts[-1] + block

        def heads(m, _):
            work = []
            for n in range(group):
                cols = [pl.ds(pl.multiple_of(k * width + (m * group + n) * HEAD, HEAD), HEAD) for k in range(3)]
                k, v = turn(mid[:most, cols[1]], slice(0, most)), mid[:most, cols[2]]
                work += [(first, cols[0], turn(mid[first : first + block, cols[0]], slice(first, first + block)), k, v) for first in firsts]
            scores = [lax.dot_general(q, k[: first + block], (((1,), (1,)), ((), ())), preferred_element_type=F32) for first, _, q, k, _ in work]
            weights, totals = [], []
            for (first, *_), s in zip(work, scores):
                seen = first + lax.broadcasted_iota(jnp.int32, s.shape, 0) >= lax.broadcasted_iota(jnp.int32, s.shape, 1)
                s = jnp.where(seen, s * HEAD**-0.5, -1e30)
                w = jnp.exp(s - s.max(-1, keepdims=True))
                totals.append(w.sum(-1, keepdims=True))
                weights.append(w.astype(BF16))
            for (first, cols, _, _, v), w, total in zip(work, weights, totals):
                mid[first : first + block, cols] = (_dot(w, v[: first + block]) * (1 / total)).astype(BF16)

        lax.fori_loop(0, width // HEAD // group, heads, None)

    def attention_unit(i, p, firsts, early, late, early_at, late_at):
        per = width // TILE
        first, size = firsts[0], len(firsts) * block

        def start(j):
            for k, w in enumerate((wq, wk, wv)):
                @pl.when(lax.div(j, per) == k)
                def _():
                    cols = pl.ds(pl.multiple_of(lax.rem(j, per) * TILE, TILE), TILE)
                    pltpu.make_async_copy(w.at[:, cols], wbuf.at[lax.rem(j, SLOTS)], wsem.at[lax.rem(j, SLOTS), 0]).start()

        def wait(j):
            pltpu.make_async_copy(wq.at[:, pl.ds(0, TILE)], wbuf.at[lax.rem(j, SLOTS)], wsem.at[lax.rem(j, SLOTS), 0]).wait()

        def work(j):
            mid[first : first + size, pl.ds(pl.multiple_of(j * TILE, TILE), TILE)] = _dot(act[:size, :], wbuf[lax.rem(j, SLOTS)]).astype(BF16)

        def ahead():
            for j in range(SLOTS - 1):
                start(j)
            if firsts == (0,):
                pltpu.make_async_copy(tables, turns, tsem).start()

        norm(x, i, first, size, gain_a, ahead)
        tiled(3 * per, SLOTS, start, wait, work, ((3 * per - SLOTS + 1, lambda: last_begin(wo)), (early_at, early), (late_at, late)))
        attend(firsts, GROUP if width // HEAD % GROUP == 0 else 1)
        pl.when(late_at >= 3 * per)(late)
        last(wo, p, first, size)

    def mlp_unit(i, p, early, late):
        part = TILE // 2
        count = ff // part

        def copies(j):
            cols = pl.ds(pl.multiple_of(j * part, part), part)
            return [pltpu.make_async_copy(w.at[:, cols], wbuf.at[lax.rem(j, SLOTS), :, pl.ds(k * part, part)], wsem.at[lax.rem(j, SLOTS), k])
                    for k, w in enumerate((w_gate, w_up))]

        def work(j):
            both = _dot(act[...], wbuf[lax.rem(j, SLOTS)])
            mid[:, pl.ds(pl.multiple_of(j * part, part), part)] = (jax.nn.silu(both[:, :part]) * both[:, part:]).astype(BF16)

        def start(j):
            for c in copies(j):
                c.start()

        def wait(j):
            for c in copies(j):
                c.wait()

        def ahead():
            for j in range(SLOTS - 1):
                start(j)
            last_begin(w_down)

        norm(out, i, 0, rows, gain_m, ahead)
        tiled(count, SLOTS, start, wait, work, ((count // 4, early), (count - 1, late)))
        last(w_down, p, 0, rows)


    def nothing():
        pass

    steps = 3 * (width // TILE)
    barrier = pltpu.get_barrier_semaphore()
    for neighbour in (left, right):
        pl.semaphore_signal(barrier, inc=1, device_id={"tp": neighbour}, device_id_type=MESH)
    attention_unit(0, 0, (0,), pltpu.make_async_copy(tables, turns, tsem).wait, nothing, steps // 2, steps)
    pl.semaphore_wait(barrier, 2)
    begin(0, True)
    attention_unit(0, 1, (block,), lambda: relay(0, True), lambda: own(0, True), EARLY[0] * steps // 16, LATE[0] * steps // 16)

    def slot(s, _):
        mlp, i = unit(s)
        p = lax.rem(s, 2)

        def early():
            when(s - 1, relay)
            when(s - 2, forward)

        def late():
            when(s - 1, own)

        when(s - 1, begin)

        @pl.when((s < units) & jnp.logical_not(mlp))
        def _():
            attention_unit(i, p, (0, block), early, late, jnp.where(s == 2, EARLY[1] * steps // 16, EARLY[2] * steps // 16),
                           jnp.where(s == 2, LATE[1] * steps // 16, LATE[2] * steps // 16))

        @pl.when((s < units) & mlp)
        def _():
            mlp_unit(i, p, early, late)

        @pl.when(s >= units)
        def _():
            early()
            late()

        when(s - 2, end)

    lax.fori_loop(2, units + 2, slot, None)


def _copy(src, dst, buf, came, left):
    batch, rows, _ = dst.shape
    part = buf.shape[1]
    places = [(i, pl.ds(r * part, part)) for i in range(batch) for r in range(rows // part)]

    def into(n):
        i, here = places[n]
        return pltpu.make_async_copy(src.at[src.shape[0] - batch + i, here], buf.at[n], came.at[n])

    def back(n):
        i, here = places[n]
        return pltpu.make_async_copy(buf.at[n], dst.at[i, here], left.at[n])

    for n in range(len(places)):
        into(n).start()
    for n in range(len(places)):
        into(n).wait()
        back(n).start()
    for n in range(len(places)):
        back(n).wait()


def layer(x, gain_a, wq, wk, wv, wo, gain_m, w_gate, w_up, w_down):
    batch, rows, d = x.shape
    width, ff = wq.shape[1], w_gate.shape[1]
    half = HEAD // 2
    angle = np.arange(rows, dtype=np.float32)[:, None] * np.power(np.float32(THETA), -np.arange(half, dtype=np.float32) / np.float32(half))
    cos, sin = np.cos(angle).astype(np.float32), np.sin(angle).astype(np.float32)
    tables = np.stack([np.concatenate([cos, cos], 1), np.concatenate([-sin, sin], 1)])
    hbm, vmem = pl.BlockSpec(memory_space=pl.ANY), pl.BlockSpec(memory_space=pltpu.VMEM)
    part = min(rows // 2, 128)
    out = pl.pallas_call(
        _layer,
        in_specs=[hbm, vmem, hbm, hbm, hbm, hbm, vmem, hbm, hbm, hbm, hbm],
        out_specs=hbm,
        out_shape=jax.ShapeDtypeStruct((2 * batch, rows, d), BF16),
        scratch_shapes=[
            pltpu.VMEM(tables.shape, F32),
            pltpu.SemaphoreType.DMA,
            pltpu.VMEM((SLOTS, d, TILE), BF16),
            pltpu.VMEM((2, max(width, ff), WIDE), BF16),
            pltpu.VMEM((rows, d), BF16),
            pltpu.VMEM((rows, max(3 * width, ff)), BF16),
            pltpu.VMEM((2, rows, d), BF16),
            pltpu.VMEM((2, 6, rows // 4, d // 2), BF16),
            pltpu.VMEM((2, rows // 4, d), BF16),
            pltpu.VMEM((2, part, d), BF16),
            pltpu.SemaphoreType.DMA((SLOTS, 2)),
            pltpu.SemaphoreType.DMA((2 * (max(width, ff) // min(width, ff)),)),
            pltpu.SemaphoreType.DMA((2,)),
            pltpu.SemaphoreType.DMA((1,)),
            pltpu.SemaphoreType.DMA((2,)),
            pltpu.SemaphoreType.DMA((2, 12)),
            pltpu.SemaphoreType.DMA((2, 12)),
        ],
        compiler_params=pltpu.CompilerParams(collective_id=0, has_side_effects=True, vmem_limit_bytes=67043328),
        name="layer",
    )(x, gain_a, wq, wk, wv, wo, gain_m, w_gate, w_up, w_down, jnp.asarray(tables))
    part = min(rows, COPIED)
    parts = batch * rows // part
    return pl.pallas_call(
        _copy,
        in_specs=[hbm],
        out_specs=hbm,
        out_shape=jax.ShapeDtypeStruct((batch, rows, d), BF16),
        scratch_shapes=[pltpu.VMEM((parts, part, d), BF16), pltpu.SemaphoreType.DMA((parts,)), pltpu.SemaphoreType.DMA((parts,))],
        compiler_params=pltpu.CompilerParams(vmem_limit_bytes=48 * 2**20),
        name="result",
    )(out)


def solution(mesh):
    tokens, whole, columns, rows_of = P("dp", None, None), P(None), P(None, "tp"), P("tp", None)
    return jax.shard_map(
        layer,
        mesh=mesh,
        in_specs=(tokens, whole, columns, columns, columns, rows_of, whole, columns, columns, rows_of),
        out_specs=tokens,
        check_vma=False,
    )
```

```python
import functools

import jax
import jax.numpy as jnp
import numpy as np
from jax import lax
from jax.experimental import pallas as pl
from jax.experimental.pallas import tpu as pltpu
from jax.sharding import PartitionSpec as P

HEAD = 128
THETA = 10000
GROUP = 5
SUBS = 2
SLOTS = 4
TILE = 256
WIDE = 512
STRIP = 16
COPIED = 512
EARLY, LATE = (8, 5, 8), (16, 14, 16)
MESH = pl.DeviceIdType.MESH
F32, BF16 = jnp.float32, jnp.bfloat16


def _dot(a, w):
    return jnp.dot(a, w, preferred_element_type=F32)


def _layer(x, gain_a, wq, wk, wv, wo, gain_m, w_gate, w_up, w_down, tables, out,
           turns, tsem, wbuf, vbuf, act, mid, term, got, fin, xin, wsem, vsem, xsem, qsem, osem, send, recv):
    batch, rows, d = x.shape
    units = 2 * batch + 1
    width, ff = wq.shape[1], w_gate.shape[1]
    block, half = rows // 2, d // 2
    me = lax.axis_index("tp")
    right, opposite, left = lax.rem(me + 1, 4), lax.rem(me + 2, 4), lax.rem(me + 3, 4)
    low, high, every = pl.ds(0, half), pl.ds(half, half), pl.ds(0, d)

    def unit(u):
        mlp = (u == batch) | (u > batch + 1)
        return mlp, jnp.where(mlp, jnp.where(u == batch, 0, u - 1 - batch), jnp.where(u == batch + 1, batch - 1, jnp.maximum(u - 1, 0)))

    def share(small):
        return (block if small else rows) // 4

    def part_of(q, small, sub):
        size = share(small) // SUBS
        return pl.ds(pl.multiple_of(q * share(small) + sub * size, size), size)

    def at(u, q, small, sub=None):
        size = share(small) // (1 if sub is None else SUBS)
        first = (u * block if small else 0) + (0 if sub is None else sub * size)
        return pl.ds(pl.multiple_of(first + q * share(small), size), size)


    def piece(u, n, small, sub):
        p = lax.rem(u, 2)
        mlp, i = unit(u)
        o = jnp.where(mlp, batch + i, i)
        to = left if n in (0, 1, 2, 6, 8, 10) else right
        some = pl.ds(sub * (share(small) // SUBS), share(small) // SUBS)
        if n < 6:
            q, cols = ((opposite, low), (left, high), (left, low), (opposite, high), (right, low), (right, high))[n]
            src, dst = term.at[p, part_of(q, small, sub), cols], got.at[p, n, some]
        elif n in (6, 7, 10, 11):
            cols = low if n in (6, 11) else high
            src, dst = fin.at[p, some, cols], out.at[o, at(u, me, small, sub), cols]
        else:
            q, cols = ((right, low), (left, high))[n - 8]
            src = dst = out.at[o, at(u, q, small, sub), cols]
        return pltpu.make_async_remote_copy(src_ref=src, dst_ref=dst, send_sem=send.at[p, n, sub], recv_sem=recv.at[p, n, sub],
                                            device_id={"tp": to}, device_id_type=MESH)

    def residual(u, small, src):
        _, i = unit(u)
        return pltpu.make_async_copy(src.at[i, at(u, me, small), every], fin.at[lax.rem(u, 2), pl.ds(0, share(small))], qsem.at[0])

    def kept(u, small):
        mlp, i = unit(u)
        p = lax.rem(u, 2)
        return pltpu.make_async_copy(fin.at[p, pl.ds(0, share(small))], out.at[jnp.where(mlp, batch + i, i), at(u, me, small), every], osem.at[p])

    def begin(u, small):
        for n in (0, 3, 1, 4):
            for sub in range(SUBS):
                piece(u, n, small, sub).start()
        if small:
            residual(u, small, x).start()
        else:
            mlp, _ = unit(u)

            @pl.when(mlp)
            def _():
                residual(u, small, out).start()

            @pl.when(jnp.logical_not(mlp))
            def _():
                residual(u, small, x).start()

    def relay(u, small):
        p = lax.rem(u, 2)
        size = share(small) // SUBS
        for sub in range(SUBS):
            for n, q, cols, after in ((0, left, low, 2), (3, right, high, 5)):
                piece(u, n, small, sub).wait_recv()

                def add(r, _):
                    here = pl.ds(pl.multiple_of(q * share(small) + sub * size + r * STRIP, STRIP), STRIP)
                    came = got[p, n, pl.ds(pl.multiple_of(sub * size + r * STRIP, STRIP), STRIP), :]
                    term[p, here, cols] = (term[p, here, cols].astype(F32) + came.astype(F32)).astype(BF16)

                lax.fori_loop(0, size // STRIP, add, None)
                piece(u, after, small, sub).start()

    def own(u, small):
        p = lax.rem(u, 2)
        size = share(small) // SUBS
        residual(u, small, x).wait()
        for sub in range(SUBS):
            for n in (1, 4, 2, 5):
                piece(u, n, small, sub).wait_recv()

            def add(r, _):
                here = pl.ds(pl.multiple_of(sub * size + r * STRIP, STRIP), STRIP)
                mine = pl.ds(pl.multiple_of(me * share(small) + sub * size + r * STRIP, STRIP), STRIP)
                for cols, a, b in ((low, 2, 4), (high, 5, 1)):
                    total = term[p, mine, cols].astype(F32) + got[p, a, here, :].astype(F32) + got[p, b, here, :].astype(F32)
                    fin[p, here, cols] = (fin[p, here, cols].astype(F32) + total).astype(BF16)

            lax.fori_loop(0, size // STRIP, add, None)
            for n in (6, 7, 10, 11):
                piece(u, n, small, sub).start()
        kept(u, small).start()

    def forward(u, small):
        for sub in range(SUBS):
            for n, after in ((6, 8), (7, 9)):
                piece(u, n, small, sub).wait_recv()
                piece(u, after, small, sub).start()
        for n in range(6):
            for sub in range(SUBS):
                piece(u, n, small, sub).wait_send()

    def end(u, small):
        for n in (10, 11, 8, 9):
            for sub in range(SUBS):
                piece(u, n, small, sub).wait_recv()
        for n in (6, 7, 10, 11, 8, 9):
            for sub in range(SUBS):
                piece(u, n, small, sub).wait_send()
        kept(u, small).wait()

    def when(u, event):
        @pl.when((u >= 0) & (u < 2))
        def _():
            event(u, True)

        @pl.when((u >= 2) & (u < units))
        def _():
            event(u, False)


    def norm(src, i, first, size, gain, then):
        part = min(xin.shape[1], size)

        def load(t):
            return pltpu.make_async_copy(src.at[i, pl.ds(pl.multiple_of(first + t * part, part), part), every],
                                         xin.at[lax.rem(t, 2), pl.ds(0, part)], xsem.at[lax.rem(t, 2)])

        load(0).start()
        if size > part:
            load(1).start()
        then()
        g = gain[...].astype(F32).reshape(1, d)

        def tile(t, _):
            @pl.when((t >= 1) & (t + 1 < size // part))
            def _():
                load(t + 1).start()

            load(t).wait()

            def strip(r, _):
                wide = xin[lax.rem(t, 2), pl.ds(pl.multiple_of(r * STRIP, STRIP), STRIP), :].astype(F32)
                scale = lax.rsqrt(jnp.mean(wide * wide, -1, keepdims=True) + 1e-6)
                act[pl.ds(pl.multiple_of(t * part + r * STRIP, STRIP), STRIP), :] = (wide * scale * g).astype(BF16)

            lax.fori_loop(0, part // STRIP, strip, None, unroll=2)

        lax.fori_loop(0, size // part, tile, None)

    def tiled(count, slots, start, wait, work, hooks=()):
        def step(j, _):
            @pl.when(j + slots - 1 < count)
            def _():
                start(j + slots - 1)

            wait(j)
            work(j)
            for when_j, hook in hooks:
                pl.when(j == when_j)(hook)

        lax.fori_loop(0, count, step, None)

    def last_slots(w):
        return 2 * (vbuf.shape[1] // w.shape[0])

    def last_at(w, j):
        slot, depth = lax.rem(j, last_slots(w)), w.shape[0]
        return lax.rem(slot, 2), pl.ds(pl.multiple_of(lax.div(slot, 2) * depth, depth), depth), slice(None)

    def last_tile(w, j):
        return pltpu.make_async_copy(w.at[:, pl.ds(pl.multiple_of(j * WIDE, WIDE), WIDE)], vbuf.at[last_at(w, j)],
                                     vsem.at[lax.rem(j, last_slots(w))])

    def last_begin(w):
        for j in range(last_slots(w) - 1):
            last_tile(w, j).start()

    def last(w, p, first, size):
        def work(j):
            term[p, :size, pl.ds(pl.multiple_of(j * WIDE, WIDE), WIDE)] = _dot(mid[first : first + size, : w.shape[0]],
                                                                               vbuf[last_at(w, j)]).astype(BF16)

        tiled(d // WIDE, last_slots(w), lambda j: last_tile(w, j).start(), lambda j: last_tile(w, j).wait(), work)

    def turn(t, where):
        t = t.astype(F32)
        return (t * turns[0, where] + pltpu.roll(t, HEAD // 2, 1) * turns[1, where]).astype(BF16)

    def attend(firsts, group):
        most = firsts[-1] + block

        def heads(m, _):
            work = []
            for n in range(group):
                cols = [pl.ds(pl.multiple_of(k * width + (m * group + n) * HEAD, HEAD), HEAD) for k in range(3)]
                k, v = turn(mid[:most, cols[1]], slice(0, most)), mid[:most, cols[2]]
                work += [(first, cols[0], turn(mid[first : first + block, cols[0]], slice(first, first + block)), k, v) for first in firsts]
            scores = [lax.dot_general(q, k[: first + block], (((1,), (1,)), ((), ())), preferred_element_type=F32) for first, _, q, k, _ in work]
            weights, totals = [], []
            for (first, *_), s in zip(work, scores):
                seen = first + lax.broadcasted_iota(jnp.int32, s.shape, 0) >= lax.broadcasted_iota(jnp.int32, s.shape, 1)
                s = jnp.where(seen, s * HEAD**-0.5, -1e30)
                w = jnp.exp(s - s.max(-1, keepdims=True))
                totals.append(w.sum(-1, keepdims=True))
                weights.append(w.astype(BF16))
            for (first, cols, _, _, v), w, total in zip(work, weights, totals):
                mid[first : first + block, cols] = (_dot(w, v[: first + block]) * (1 / total)).astype(BF16)

        lax.fori_loop(0, width // HEAD // group, heads, None)

    def attention_unit(i, p, firsts, early, late, early_at, late_at):
        per = width // TILE
        first, size = firsts[0], len(firsts) * block

        def start(j):
            for k, w in enumerate((wq, wk, wv)):
                @pl.when(lax.div(j, per) == k)
                def _():
                    cols = pl.ds(pl.multiple_of(lax.rem(j, per) * TILE, TILE), TILE)
                    pltpu.make_async_copy(w.at[:, cols], wbuf.at[lax.rem(j, SLOTS)], wsem.at[lax.rem(j, SLOTS), 0]).start()

        def wait(j):
            pltpu.make_async_copy(wq.at[:, pl.ds(0, TILE)], wbuf.at[lax.rem(j, SLOTS)], wsem.at[lax.rem(j, SLOTS), 0]).wait()

        def work(j):
            mid[first : first + size, pl.ds(pl.multiple_of(j * TILE, TILE), TILE)] = _dot(act[:size, :], wbuf[lax.rem(j, SLOTS)]).astype(BF16)

        def ahead():
            for j in range(SLOTS - 1):
                start(j)
            if firsts == (0,):
                pltpu.make_async_copy(tables, turns, tsem).start()

        norm(x, i, first, size, gain_a, ahead)
        tiled(3 * per, SLOTS, start, wait, work, ((3 * per - SLOTS + 1, lambda: last_begin(wo)), (early_at, early), (late_at, late)))
        attend(firsts, GROUP if width // HEAD % GROUP == 0 else 1)
        pl.when(late_at >= 3 * per)(late)
        last(wo, p, first, size)

    def mlp_unit(i, p, early, late):
        part = TILE // 2
        count = ff // part

        def copies(j):
            cols = pl.ds(pl.multiple_of(j * part, part), part)
            return [pltpu.make_async_copy(w.at[:, cols], wbuf.at[lax.rem(j, SLOTS), :, pl.ds(k * part, part)], wsem.at[lax.rem(j, SLOTS), k])
                    for k, w in enumerate((w_gate, w_up))]

        def work(j):
            both = _dot(act[...], wbuf[lax.rem(j, SLOTS)])
            mid[:, pl.ds(pl.multiple_of(j * part, part), part)] = (jax.nn.silu(both[:, :part]) * both[:, part:]).astype(BF16)

        def start(j):
            for c in copies(j):
                c.start()

        def wait(j):
            for c in copies(j):
                c.wait()

        def ahead():
            for j in range(SLOTS - 1):
                start(j)
            last_begin(w_down)

        norm(out, i, 0, rows, gain_m, ahead)
        tiled(count, SLOTS, start, wait, work, ((count // 4, early), (count - 1, late)))
        last(w_down, p, 0, rows)


    def nothing():
        pass

    steps = 3 * (width // TILE)
    barrier = pltpu.get_barrier_semaphore()
    for neighbour in (left, right):
        pl.semaphore_signal(barrier, inc=1, device_id={"tp": neighbour}, device_id_type=MESH)
    attention_unit(0, 0, (0,), pltpu.make_async_copy(tables, turns, tsem).wait, nothing, steps // 2, steps)
    pl.semaphore_wait(barrier, 2)
    begin(0, True)
    attention_unit(0, 1, (block,), lambda: relay(0, True), lambda: own(0, True), EARLY[0] * steps // 16, LATE[0] * steps // 16)

    def slot(s, _):
        mlp, i = unit(s)
        p = lax.rem(s, 2)

        def early():
            when(s - 1, relay)
            when(s - 2, forward)

        def late():
            when(s - 1, own)

        when(s - 1, begin)

        @pl.when((s < units) & jnp.logical_not(mlp))
        def _():
            attention_unit(i, p, (0, block), early, late, jnp.where(s == 2, EARLY[1] * steps // 16, EARLY[2] * steps // 16),
                           jnp.where(s == 2, LATE[1] * steps // 16, LATE[2] * steps // 16))

        @pl.when((s < units) & mlp)
        def _():
            mlp_unit(i, p, early, late)

        @pl.when(s >= units)
        def _():
            early()
            late()

        when(s - 2, end)

    lax.fori_loop(2, units + 2, slot, None)


def _copy(src, dst):
    dst[...] = src[...]


def layer(x, gain_a, wq, wk, wv, wo, gain_m, w_gate, w_up, w_down):
    batch, rows, d = x.shape
    width, ff = wq.shape[1], w_gate.shape[1]
    half = HEAD // 2
    angle = np.arange(rows, dtype=np.float32)[:, None] * np.power(np.float32(THETA), -np.arange(half, dtype=np.float32) / np.float32(half))
    cos, sin = np.cos(angle).astype(np.float32), np.sin(angle).astype(np.float32)
    tables = np.stack([np.concatenate([cos, cos], 1), np.concatenate([-sin, sin], 1)])
    hbm, vmem = pl.BlockSpec(memory_space=pl.ANY), pl.BlockSpec(memory_space=pltpu.VMEM)
    part = min(rows // 2, 128)
    out = pl.pallas_call(
        _layer,
        in_specs=[hbm, vmem, hbm, hbm, hbm, hbm, vmem, hbm, hbm, hbm, hbm],
        out_specs=hbm,
        out_shape=jax.ShapeDtypeStruct((2 * batch, rows, d), BF16),
        scratch_shapes=[
            pltpu.VMEM(tables.shape, F32),
            pltpu.SemaphoreType.DMA,
            pltpu.VMEM((SLOTS, d, TILE), BF16),
            pltpu.VMEM((2, max(width, ff), WIDE), BF16),
            pltpu.VMEM((rows, d), BF16),
            pltpu.VMEM((rows, max(3 * width, ff)), BF16),
            pltpu.VMEM((2, rows, d), BF16),
            pltpu.VMEM((2, 6, rows // 4, d // 2), BF16),
            pltpu.VMEM((2, rows // 4, d), BF16),
            pltpu.VMEM((2, part, d), BF16),
            pltpu.SemaphoreType.DMA((SLOTS, 2)),
            pltpu.SemaphoreType.DMA((2 * (max(width, ff) // min(width, ff)),)),
            pltpu.SemaphoreType.DMA((2,)),
            pltpu.SemaphoreType.DMA((1,)),
            pltpu.SemaphoreType.DMA((2,)),
            pltpu.SemaphoreType.DMA((2, 12, SUBS)),
            pltpu.SemaphoreType.DMA((2, 12, SUBS)),
        ],
        compiler_params=pltpu.CompilerParams(collective_id=0, has_side_effects=True, vmem_limit_bytes=67043328),
        name="layer",
    )(x, gain_a, wq, wk, wv, wo, gain_m, w_gate, w_up, w_down, jnp.asarray(tables))
    strip = (1, min(rows, COPIED), d)
    return pl.pallas_call(
        _copy,
        grid=(batch, rows // strip[1]),
        in_specs=[pl.BlockSpec(strip, lambda i, r: (batch + i, r, 0))],
        out_specs=pl.BlockSpec(strip, lambda i, r: (i, r, 0)),
        out_shape=jax.ShapeDtypeStruct((batch, rows, d), BF16),
        name="result",
    )(out)


def solution(mesh):
    tokens, whole, columns, rows_of = P("dp", None, None), P(None), P(None, "tp"), P("tp", None)
    return jax.shard_map(
        layer,
        mesh=mesh,
        in_specs=(tokens, whole, columns, columns, columns, rows_of, whole, columns, columns, rows_of),
        out_specs=tokens,
        check_vma=False,
    )
```
